32 devices in a mesh: kv: 16 (over z, y, x), head: 2 (over core).
Axes of the slice: x: 2, y: 2, z: 4, core: 2. Of those that a mesh axis runs over, the one named last changes fastest.
Arguments:
- queries: bfloat16 [8, 256, 128], P('head', 'kv'), may hold values from -384 to 384
- key_cache: bfloat16 [4096, 8, 128, 128], P('kv', 'head'), may hold values from -6 to 6
- value_cache: bfloat16 [4096, 8, 128, 128], P('kv', 'head'), may hold values from -6 to 6
- key_new: bfloat16 [32, 8, 128], P(None, 'head'), may hold values from -6 to 6
- value_new: bfloat16 [32, 8, 128], P(None, 'head'), may hold values from -6 to 6
- lengths: int32 [32], replicated, may hold values from 2 to 16385, as said below
- page_table: int32 [4096], replicated, may hold values from 0 to 4095, each once
Outputs:
- attended: bfloat16 [8, 256, 128], P('head', 'kv')
The draws below stay inside these ranges and needn't reach their ends.
Inputs may be any that keep to these rules, and one draw needn't show every extreme that they name: The cache holds the first lengths[s] - 1 tokens of sequence s; some sequence has the largest length. `page_table`: every page appears once; page g lies on kv index g // 256.
All inputs are finite; a program needn't handle non-finite values.
Results may differ from the reference program's by a relative error of at most 0.0025.
Values may be sent and summed in bfloat16 or wider, within the bound.
A program may use at most 128 MiB of HBM per device.

```python
import math
import jax
import jax.numpy as jnp
from jax import lax

QH = 64
KVH = 8
HD = 128
PAGE = 128
MAXP = 128
SEQS = 32
PAGES = 4096


def draw_queries(key, part):
    normal_part = jax.random.normal(jax.random.fold_in(key, 11), (KVH, SEQS * (QH // KVH), HD), jnp.float32)
    values = jnp.clip(normal_part * 2.0, -8.0, 8.0)
    return values.astype(jnp.bfloat16)


def draw_lengths(key, part):
    most = MAXP * PAGE + 1
    values = jax.random.randint(jax.random.fold_in(key, 21), (SEQS,), 2, most + 1, jnp.int32)
    chosen = jax.random.randint(jax.random.fold_in(key, 22), (), 0, SEQS, jnp.int32)
    return jnp.where(jnp.arange(SEQS, dtype=jnp.int32) == chosen, most, values).astype(jnp.int32)


def block_levels(rng, shape, shards, low, largest):
    level, own = 1.0, jax.random.fold_in(rng, 6)
    for axis_at, shards_of in shards:
        draws = jnp.exp(jax.random.uniform(jax.random.fold_in(own, axis_at), (shards_of,), jnp.float32, low / len(shards), largest / len(shards)))
        level = level * jnp.repeat(draws, shape[axis_at] // shards_of).reshape([-1 if axis == axis_at else 1 for axis in range(len(shape))])
    return level


def noise(rng, dims, width, most, pieces=(), held_as=jnp.bfloat16):
    gain = block_levels(rng, dims, pieces, -0.22, 0.18) if pieces else 1.0
    entries = jax.random.normal(rng, dims, jnp.float32) * width * gain
    return jnp.minimum(jnp.maximum(entries, -most), most).astype(held_as)


def setup_inputs(seed: int = 0) -> dict:
    key_of = jax.random.split(jax.random.key(seed), 8)
    queries = draw_queries(jax.random.fold_in(key_of[7], 71), 0)
    key_cache = noise(key_of[1], (PAGES, KVH, PAGE, HD), 1.0, 6.0, ((0, 16), (1, 2)))
    value_cache = noise(key_of[2], (PAGES, KVH, PAGE, HD), 1.0, 6.0, ((0, 16), (1, 2)))
    key_new = noise(key_of[3], (SEQS, KVH, HD), 1.0, 6.0, ((1, 2),))
    value_new = noise(key_of[4], (SEQS, KVH, HD), 1.0, 6.0, ((1, 2),))
    lengths = draw_lengths(jax.random.fold_in(key_of[7], 71), 0)
    page_table = jax.random.permutation(key_of[6], PAGES).astype(jnp.int32)
    return {"queries": queries, "key_cache": key_cache, "value_cache": value_cache, "key_new": key_new, "value_new": value_new, "lengths": lengths, "page_table": page_table}


LOWEST_SCORE = -1e+30

def finish(cache_max, cache_sum, cache_out, query_wide, fresh_key, fresh_value, score_scale):
    new_score = lax.optimization_barrier(jnp.sum(query_wide * fresh_key.astype(jnp.float32), axis=-1)) * score_scale
    highest = jnp.maximum(cache_max, new_score)
    old_part = jnp.exp(cache_max - highest)
    new_part = jnp.exp(new_score - highest)
    numerator = cache_out * old_part[..., None] + new_part[..., None] * fresh_value.astype(jnp.float32)
    denominator = cache_sum * old_part + new_part
    return (numerator / denominator[..., None]).astype(jnp.bfloat16)

def reference(queries, key_cache, value_cache, key_new, value_new, lengths, page_table):
    seq_count = lengths.shape[0]
    kv_count = queries.shape[0]
    head_width = queries.shape[2]
    group_size = queries.shape[1] // seq_count
    page_total = key_cache.shape[0]
    page_len = key_cache.shape[2]
    page_slots = page_total // seq_count
    score_scale = 1.0 / math.sqrt(head_width)
    table = page_table.reshape(seq_count, page_slots).astype(jnp.int32)
    grouped = jnp.transpose(queries.reshape(kv_count, seq_count, group_size, head_width), (1, 0, 2, 3))
    offsets = jnp.arange(page_slots, dtype=jnp.int32)[:, None] * page_len + jnp.arange(page_len, dtype=jnp.int32)[None, :]

    def one_sequence(packed):
        query_rows, page_ids, length, fresh_key, fresh_value = packed
        keys = key_cache[page_ids].astype(jnp.float32)
        values = value_cache[page_ids].astype(jnp.float32)
        query_wide = query_rows.astype(jnp.float32)
        scores = jnp.einsum('gqd,mgtd->mgqt', query_wide, keys, precision=lax.Precision.HIGHEST) * score_scale
        in_cache = (offsets < length - 1)[:, None, None, :]
        masked = jnp.where(in_cache, scores, LOWEST_SCORE)
        page_max = lax.optimization_barrier(jnp.max(masked, axis=3))
        weights = jnp.where(in_cache, jnp.exp(masked - page_max[..., None]), 0.0)
        page_sum = lax.optimization_barrier(jnp.sum(weights, axis=3))
        rounded = lax.optimization_barrier(weights.astype(jnp.bfloat16)).astype(jnp.float32)
        page_out = jnp.einsum('mgqt,mgtd->mgqd', rounded, values, precision=lax.Precision.HIGHEST)
        cache_max = lax.optimization_barrier(jnp.max(page_max, axis=0))
        factor = jnp.exp(page_max - cache_max[None])
        cache_sum = lax.optimization_barrier(jnp.sum(page_sum * factor, axis=0))
        cache_out = lax.optimization_barrier(jnp.sum(page_out * factor[..., None], axis=0))
        return finish(cache_max, cache_sum, cache_out, query_wide, fresh_key[:, None, :], fresh_value[:, None, :], score_scale)
    result = lax.map(one_sequence, (grouped, table, lengths.astype(jnp.int32), key_new, value_new))
    return jnp.transpose(result, (1, 0, 2, 3)).reshape(kv_count, seq_count * group_size, head_width)
```

```python
import functools
import math

import jax
import jax.numpy as jnp
from jax import lax
from jax.experimental import pallas as pl
from jax.experimental.pallas import tpu as pltpu
from jax.sharding import PartitionSpec as P

LOWEST_SCORE = -1e30
MESH = pl.DeviceIdType.MESH
VMEM = pltpu.VMEM

GROUP = 8
RING = 4

_dot = functools.partial(lax.dot_general, preferred_element_type=jnp.float32)
NT = (((1,), (1,)), ((), ()))
NN = (((1,), (0,)), ((), ()))


def greet(n, me):
    barrier = pltpu.get_barrier_semaphore()
    for k in range(1, n):
        pl.semaphore_signal(
            barrier, inc=1, device_id={"kv": lax.rem(me + k, n)}, device_id_type=MESH
        )
    pl.semaphore_wait(barrier, n - 1)


def gather_kernel(n, x_ref, all_ref, send_sem, recv_sem, own_sem):
    me = lax.axis_index("kv")
    own = pltpu.make_async_copy(x_ref, all_ref.at[me], own_sem)
    own.start()
    greet(n, me)
    copies = []
    for k in range(1, n):
        copy = pltpu.make_async_remote_copy(
            src_ref=x_ref,
            dst_ref=all_ref.at[me],
            send_sem=send_sem.at[k],
            recv_sem=recv_sem.at[me],
            device_id={"kv": lax.rem(me + k, n)},
            device_id_type=MESH,
        )
        copy.start()
        copies.append(copy)
    own.wait()
    for k in range(1, n):
        source = lax.rem(me + k, n)
        pltpu.make_async_remote_copy(
            src_ref=x_ref,
            dst_ref=all_ref.at[source],
            send_sem=send_sem.at[k],
            recv_sem=recv_sem.at[source],
            device_id={"kv": source},
            device_id_type=MESH,
        ).wait_recv()
    for copy in copies:
        copy.wait_send()


def list_kernel(pages_here, page_len, table_ref, length_ref, list_ref):
    me = lax.axis_index("kv")
    seqs, slots = table_ref.shape
    listed = list_ref.shape[1]
    page = table_ref[...] - me * pages_here
    tokens = length_ref[...] - 1 - lax.broadcasted_iota(jnp.int32, (seqs, slots), 1) * page_len
    wanted = (page >= 0) & (page < pages_here) & (tokens > 0)
    flag = jnp.where(wanted, 1.0, 0.0)
    upto = jnp.where(
        lax.broadcasted_iota(jnp.int32, (slots, slots), 0)
        <= lax.broadcasted_iota(jnp.int32, (slots, slots), 1),
        1.0,
        0.0,
    ).astype(jnp.bfloat16)
    inside = _dot(flag.astype(jnp.bfloat16), upto, NN)
    total = jnp.broadcast_to(jnp.sum(flag, axis=1, keepdims=True), (seqs, slots))
    before = jnp.where(
        lax.broadcasted_iota(jnp.int32, (seqs, seqs), 1)
        < lax.broadcasted_iota(jnp.int32, (seqs, seqs), 0),
        1.0,
        0.0,
    ).astype(jnp.bfloat16)
    offset = _dot(before, total.astype(jnp.bfloat16), NN)
    rank = jnp.where(wanted, inside + offset - 1.0, -1.0).astype(jnp.int32)
    wide = jnp.where(wanted, page, 0).astype(jnp.float32)
    held = jnp.where(wanted, jnp.clip(tokens, 0, page_len), 0).astype(jnp.float32)
    row = lax.broadcasted_iota(jnp.int32, (8, slots), 0)
    slot = lax.broadcasted_iota(jnp.int32, (8, slots), 1).astype(jnp.float32)
    place = lax.broadcasted_iota(jnp.int32, (listed, slots), 0)
    out = jnp.zeros((8, listed), jnp.float32)
    for s in range(seqs):
        values = jnp.where(
            row == 0,
            float(s),
            jnp.where(
                row == 1,
                slot,
                jnp.where(
                    row == 2,
                    jnp.broadcast_to(wide[s : s + 1], (8, slots)),
                    jnp.where(row == 3, jnp.broadcast_to(held[s : s + 1], (8, slots)), 0.0),
                ),
            ),
        ).astype(jnp.bfloat16)
        chosen = jnp.where(
            place == jnp.broadcast_to(rank[s : s + 1], (listed, slots)), 1.0, 0.0
        ).astype(jnp.bfloat16)
        out = out + _dot(values, chosen, NT)
    count = jnp.sum(jnp.sum(flag, axis=1, keepdims=True), axis=0, keepdims=True)
    out = jnp.where(
        lax.broadcasted_iota(jnp.int32, (8, listed), 0) == 4,
        jnp.broadcast_to(count, (8, listed)),
        out,
    )
    list_ref[...] = out.astype(jnp.int32)


def attend_kernel(
    group_rows,
    blocks,
    list_ref,
    q_ref,
    keys,
    values,
    out_ref,
    q_wide,
    key_buf,
    value_buf,
    best,
    weight,
    total,
    key_sem,
    value_sem,
):
    heads, page_len, width = key_buf.shape[2:]
    seqs = q_wide.shape[0]
    per_block = seqs // blocks
    scale2 = math.log2(math.e) / math.sqrt(width)
    count = list_ref[4, 0]
    groups = (count + GROUP - 1) // GROUP

    def copies(g, i):
        at = g * GROUP + i
        page = list_ref[2, at]
        slot = lax.rem(g, RING)
        return (
            pltpu.make_async_copy(keys.at[page], key_buf.at[slot, i], key_sem.at[slot, i]),
            pltpu.make_async_copy(values.at[page], value_buf.at[slot, i], value_sem.at[slot, i]),
        )

    def start(g):
        for i in range(GROUP):
            for copy in copies(g, i):
                copy.start()

    for g in range(RING - 1):
        pl.when(g < groups)(functools.partial(start, g))

    best[...] = jnp.full(best.shape, LOWEST_SCORE, jnp.float32)
    weight[...] = jnp.zeros(weight.shape, jnp.float32)
    total[...] = jnp.zeros(total.shape, jnp.float32)
    if q_ref.ndim == 4 and q_ref.shape[2] % group_rows == 0:
        each = q_ref.shape[2] // group_rows
        for d in range(q_ref.shape[0]):
            for h in range(heads):
                block = q_ref[d, h].astype(jnp.float32)
                for j in range(each):
                    q_wide[d * each + j, h] = block[j * group_rows : (j + 1) * group_rows]
    else:
        for d in range(q_ref.shape[0]):
            for h in range(heads):
                rows = q_ref.shape[2]
                parts = group_rows // rows
                q_wide[d // parts, h, (d % parts) * rows : (d % parts + 1) * rows] = q_ref[
                    d, h
                ].astype(jnp.float32)

    lane = lax.broadcasted_iota(jnp.int32, (group_rows, page_len), 1)

    def step(g, carry):
        pl.when(g + RING - 1 < groups)(lambda: start(g + RING - 1))
        slot = lax.rem(g, RING)
        for i in range(GROUP):
            for copy in copies(g, i):
                copy.wait()
        seq = [list_ref[0, g * GROUP + i] for i in range(GROUP)]
        inside = [lane < list_ref[3, g * GROUP + i] for i in range(GROUP)]
        both = [(i, pair) for i in range(GROUP) for pair in range(0, heads, 2)]
        each = [(i, h) for i in range(GROUP) for h in range(heads)]
        scores = {}
        for i, pair in both:
            q2 = q_wide[seq[i], pair : pair + 2].reshape(2 * group_rows, width)
            k2 = key_buf[slot, i, pair : pair + 2].reshape(2 * page_len, width)
            found = _dot(q2.astype(jnp.bfloat16), k2, NT)
            for e in range(2):
                scores[i, pair + e] = found[
                    e * group_rows : (e + 1) * group_rows, e * page_len : (e + 1) * page_len
                ]
        tops, lines = {}, {}
        for i, h in each:
            sc = jnp.where(inside[i], scores[i, h], LOWEST_SCORE)
            scores[i, h] = sc
            tops[i, h] = jnp.broadcast_to(jnp.max(sc, axis=1, keepdims=True), sc.shape)
        for i, h in each:
            lines[i, h] = jnp.where(
                inside[i], jnp.exp2((scores[i, h] - tops[i, h]) * scale2), 0.0
            )
        outs = {}
        for i, pair in both:
            w2 = jnp.concatenate([lines[i, pair], lines[i, pair + 1]], axis=0)
            v2 = jnp.concatenate(
                [value_buf[slot, i, pair], value_buf[slot, i, pair + 1]], axis=1
            )
            found = _dot(w2.astype(jnp.bfloat16), v2, NN)
            for e in range(2):
                outs[i, pair + e] = found[
                    e * group_rows : (e + 1) * group_rows, e * width : (e + 1) * width
                ]
        for i, h in each:
            s = seq[i]
            old = best[s, h]
            new = jnp.maximum(old, tops[i, h])
            keep = jnp.exp2((old - new) * scale2)
            add = jnp.exp2((tops[i, h] - new) * scale2)
            best[s, h] = new
            weight[s, h] = weight[s, h] * keep + lines[i, h] * add
            total[s, h] = total[s, h] * keep + outs[i, h] * add
        return carry

    lax.fori_loop(0, groups, step, 0)

    stat_lane = lax.broadcasted_iota(jnp.int32, (group_rows, width), 1)
    columns = heads * per_block
    for b in range(blocks):
        stats = jnp.zeros((group_rows, width), jnp.float32)
        for j in range(per_block):
            s = b * per_block + j
            for h in range(heads):
                at = h * per_block + j
                out_ref[b, at] = total[s, h]
                mass = jnp.sum(weight[s, h], axis=1, keepdims=True)
                stats = jnp.where(stat_lane == at, best[s, h], stats)
                stats = jnp.where(
                    stat_lane == columns + at, jnp.broadcast_to(mass, stats.shape), stats
                )
        out_ref[b, columns] = stats


def exchange_kernel(
    n, parts, part_ref, q_ref, key_ref, value_ref, out_ref, held, send_sem, recv_sem, own_sem
):
    me = lax.axis_index("kv")
    tiles, group_rows, width = held.shape[1:]
    columns = tiles - 1
    heads = q_ref.shape[0]
    per_block = columns // heads
    own = pltpu.make_async_copy(part_ref.at[me // parts], held.at[me], own_sem)
    own.start()
    greet(n, me)
    copies = []
    for k in range(1, n):
        other = lax.rem(me + k, n)
        copy = pltpu.make_async_remote_copy(
            src_ref=part_ref.at[other // parts],
            dst_ref=held.at[me],
            send_sem=send_sem.at[k],
            recv_sem=recv_sem.at[me],
            device_id={"kv": other},
            device_id_type=MESH,
        )
        copy.start()
        copies.append(copy)
    own.wait()
    for k in range(1, n):
        source = lax.rem(me + k, n)
        pltpu.make_async_remote_copy(
            src_ref=part_ref.at[source // parts],
            dst_ref=held.at[source],
            send_sem=send_sem.at[k],
            recv_sem=recv_sem.at[source],
            device_id={"kv": source},
            device_id_type=MESH,
        ).wait_recv()
    scale = 1.0 / math.sqrt(width)
    scale2 = scale * math.log2(math.e)
    top = held[0, columns]
    for d in range(1, n):
        top = jnp.maximum(top, held[d, columns])
    mass = jnp.zeros_like(top)
    sums = [jnp.zeros_like(top) for _ in range(columns)]
    for d in range(n):
        stats = held[d, columns]
        factor = jnp.exp2((stats - top) * scale2)
        mass = mass + stats * pltpu.roll(factor, columns, 1)
        for c in range(columns):
            sums[c] = sums[c] + held[d, c] * jnp.broadcast_to(factor[:, c : c + 1], top.shape)
    for h in range(heads):
        wide = q_ref[h].astype(jnp.float32)
        results = []
        for j in range(per_block):
            c = h * per_block + j
            s = (me // parts) * per_block + j
            rows = slice(j * group_rows, (j + 1) * group_rows) if parts == 1 else slice(None)
            query = wide[rows]
            shape = query.shape
            fresh_key = jnp.broadcast_to(key_ref[s][h : h + 1].astype(jnp.float32), shape)
            fresh_value = jnp.broadcast_to(value_ref[s][h : h + 1].astype(jnp.float32), shape)
            new = jnp.broadcast_to(jnp.sum(query * fresh_key, axis=1, keepdims=True), shape)

            def mine(x):
                if parts == 1:
                    return x
                size = group_rows // parts
                picked = x[:size]
                for p in range(1, parts):
                    picked = jnp.where(
                        lax.rem(me, parts) == p, x[p * size : (p + 1) * size], picked
                    )
                return picked

            old = mine(jnp.broadcast_to(top[:, c : c + 1], top.shape))
            old_mass = mine(jnp.broadcast_to(mass[:, columns + c : columns + c + 1], top.shape))
            old_sum = mine(sums[c])
            highest = jnp.maximum(old, new)
            old_part = jnp.exp2((old - highest) * scale2)
            new_part = jnp.exp2((new - highest) * scale2)
            results.append(
                (old_sum * old_part + new_part * fresh_value) / (old_mass * old_part + new_part)
            )
        out_ref[h] = jnp.concatenate(results, axis=0).astype(out_ref.dtype)
    for copy in copies:
        copy.wait_send()


def on_device(n, queries, key_cache, value_cache, key_new, value_new, lengths, page_table):
    heads, local_rows, width = queries.shape
    seqs = lengths.shape[0]
    slots = page_table.shape[0] // seqs
    pages_here, _, page_len, _ = key_cache.shape
    group_rows = local_rows * n // seqs
    parts = max(1, group_rows // local_rows)
    blocks = n // parts
    tiles = heads * (seqs // blocks) + 1
    listed = -(-pages_here // 128) * 128 + 128
    vmem = pl.BlockSpec(memory_space=VMEM)
    smem = pl.BlockSpec(memory_space=pltpu.SMEM)
    hbm = pl.BlockSpec(memory_space=pl.ANY)

    pages = pl.pallas_call(
        functools.partial(list_kernel, pages_here, page_len),
        out_shape=jax.ShapeDtypeStruct((8, listed), jnp.int32),
        in_specs=[vmem] * 2,
        out_specs=vmem,
        name="pages_in_cache",
    )(page_table.reshape(seqs, slots), lengths.reshape(seqs, 1))

    every_query = pl.pallas_call(
        functools.partial(gather_kernel, n),
        out_shape=jax.ShapeDtypeStruct((n,) + queries.shape, queries.dtype),
        in_specs=[vmem],
        out_specs=vmem,
        scratch_shapes=[
            pltpu.SemaphoreType.DMA((n,)),
            pltpu.SemaphoreType.DMA((n,)),
            pltpu.SemaphoreType.DMA,
        ],
        compiler_params=pltpu.CompilerParams(collective_id=0, has_side_effects=True),
        name="gather_queries",
    )(queries)

    part = pl.pallas_call(
        functools.partial(attend_kernel, group_rows, blocks),
        out_shape=jax.ShapeDtypeStruct((blocks, tiles, group_rows, width), jnp.float32),
        in_specs=[smem, vmem, hbm, hbm],
        out_specs=vmem,
        scratch_shapes=[
            VMEM((seqs, heads, group_rows, width), jnp.float32),
            VMEM((RING, GROUP, heads, page_len, width), key_cache.dtype),
            VMEM((RING, GROUP, heads, page_len, width), value_cache.dtype),
            VMEM((seqs, heads, group_rows, page_len), jnp.float32),
            VMEM((seqs, heads, group_rows, page_len), jnp.float32),
            VMEM((seqs, heads, group_rows, width), jnp.float32),
            pltpu.SemaphoreType.DMA((RING, GROUP)),
            pltpu.SemaphoreType.DMA((RING, GROUP)),
        ],
        compiler_params=pltpu.CompilerParams(vmem_limit_bytes=48 * 1024 * 1024),
        name="attend_pages",
    )(pages, every_query, key_cache, value_cache)

    return pl.pallas_call(
        functools.partial(exchange_kernel, n, parts),
        out_shape=jax.ShapeDtypeStruct(queries.shape, jnp.bfloat16),
        in_specs=[vmem] * 4,
        out_specs=vmem,
        scratch_shapes=[
            VMEM((n, tiles, group_rows, width), jnp.float32),
            pltpu.SemaphoreType.DMA((n,)),
            pltpu.SemaphoreType.DMA((n,)),
            pltpu.SemaphoreType.DMA,
        ],
        compiler_params=pltpu.CompilerParams(collective_id=1, has_side_effects=True),
        name="exchange_and_finish",
    )(part, queries, key_new, value_new)


def solution(mesh):
    placed = (
        P("head", "kv", None),
        P("kv", "head", None, None),
        P("kv", "head", None, None),
        P(None, "head", None),
        P(None, "head", None),
        P(),
        P(),
    )
    return jax.shard_map(
        functools.partial(on_device, mesh.shape["kv"]),
        mesh=mesh,
        in_specs=placed,
        out_specs=P("head", "kv", None),
        check_vma=False,
    )
```

```python
import functools
import math

import jax
import jax.numpy as jnp
from jax import lax
from jax.experimental import pallas as pl
from jax.experimental.pallas import tpu as pltpu
from jax.sharding import PartitionSpec as P

LOWEST_SCORE = -1e30
MESH = pl.DeviceIdType.MESH
VMEM = pltpu.VMEM

GROUP = 8
RING = 4

_dot = functools.partial(lax.dot_general, preferred_element_type=jnp.float32)
NT = (((1,), (1,)), ((), ()))
NN = (((1,), (0,)), ((), ()))


def greet(peers):
    barrier = pltpu.get_barrier_semaphore()
    for peer in peers:
        pl.semaphore_signal(barrier, inc=1, device_id={"kv": peer}, device_id_type=MESH)
    pl.semaphore_wait(barrier, len(peers))


def gather_kernel(
    n,
    pages_here,
    page_len,
    x_ref,
    table_ref,
    length_ref,
    all_ref,
    list_ref,
    send_sem,
    recv_sem,
    own_sem,
):
    me = lax.axis_index("kv")
    own = pltpu.make_async_copy(x_ref, all_ref.at[me], own_sem)
    own.start()
    greet([lax.rem(me + k, n) for k in range(1, n)])
    copies = []
    for k in range(1, n):
        copy = pltpu.make_async_remote_copy(
            src_ref=x_ref,
            dst_ref=all_ref.at[me],
            send_sem=send_sem.at[k],
            recv_sem=recv_sem.at[me],
            device_id={"kv": lax.rem(me + k, n)},
            device_id_type=MESH,
        )
        copy.start()
        copies.append(copy)
    list_pages(me, pages_here, page_len, table_ref, length_ref, list_ref)
    own.wait()
    for k in range(1, n):
        source = lax.rem(me + k, n)
        pltpu.make_async_remote_copy(
            src_ref=x_ref,
            dst_ref=all_ref.at[source],
            send_sem=send_sem.at[k],
            recv_sem=recv_sem.at[source],
            device_id={"kv": source},
            device_id_type=MESH,
        ).wait_recv()
    for copy in copies:
        copy.wait_send()


def list_pages(me, pages_here, page_len, table_ref, length_ref, list_ref):
    seqs, slots = table_ref.shape
    listed = list_ref.shape[1]
    page = table_ref[...] - me * pages_here
    line = lax.broadcasted_iota(jnp.int32, (seqs, slots), 0)
    length = jnp.zeros((seqs, slots), jnp.int32)
    for s in range(seqs):
        length = jnp.where(line == s, length_ref[s], length)
    tokens = length - 1 - lax.broadcasted_iota(jnp.int32, (seqs, slots), 1) * page_len
    wanted = (page >= 0) & (page < pages_here) & (tokens > 0)
    flag = jnp.where(wanted, 1.0, 0.0)
    upto = jnp.where(
        lax.broadcasted_iota(jnp.int32, (slots, slots), 0)
        <= lax.broadcasted_iota(jnp.int32, (slots, slots), 1),
        1.0,
        0.0,
    ).astype(jnp.bfloat16)
    inside = _dot(flag.astype(jnp.bfloat16), upto, NN)
    total = jnp.broadcast_to(jnp.sum(flag, axis=1, keepdims=True), (seqs, slots))
    before = jnp.where(
        lax.broadcasted_iota(jnp.int32, (seqs, seqs), 1)
        < lax.broadcasted_iota(jnp.int32, (seqs, seqs), 0),
        1.0,
        0.0,
    ).astype(jnp.bfloat16)
    offset = _dot(before, total.astype(jnp.bfloat16), NN)
    rank = jnp.where(wanted, inside + offset - 1.0, -1.0).astype(jnp.int32)
    wide = jnp.where(wanted, page, 0).astype(jnp.float32)
    held = jnp.where(wanted, jnp.minimum(tokens, page_len), 0).astype(jnp.float32)
    row = lax.broadcasted_iota(jnp.int32, (8, slots), 0)
    slot = lax.broadcasted_iota(jnp.int32, (8, slots), 1).astype(jnp.float32)
    place = lax.broadcasted_iota(jnp.int32, (listed, slots), 0)
    out = jnp.zeros((8, listed), jnp.float32)
    for s in range(seqs):
        values = jnp.where(
            row == 0,
            float(s),
            jnp.where(
                row == 1,
                slot,
                jnp.where(
                    row == 2,
                    jnp.broadcast_to(wide[s : s + 1], (8, slots)),
                    jnp.where(row == 3, jnp.broadcast_to(held[s : s + 1], (8, slots)), 0.0),
                ),
            ),
        ).astype(jnp.bfloat16)
        chosen = jnp.where(
            place == jnp.broadcast_to(rank[s : s + 1], (listed, slots)), 1.0, 0.0
        ).astype(jnp.bfloat16)
        out = out + _dot(values, chosen, NT)
    count = jnp.sum(jnp.sum(flag, axis=1, keepdims=True), axis=0, keepdims=True)
    out = jnp.where(
        lax.broadcasted_iota(jnp.int32, (8, listed), 0) == 4,
        jnp.broadcast_to(count, (8, listed)),
        out,
    )
    list_ref[...] = out.astype(jnp.int32)


def attend_kernel(
    group_rows,
    blocks,
    list_ref,
    q_ref,
    keys,
    values,
    out_ref,
    q_wide,
    key_buf,
    value_buf,
    best,
    weight,
    total,
    key_sem,
    value_sem,
):
    heads, page_len, width = key_buf.shape[2:]
    seqs = q_wide.shape[0]
    per_block = seqs // blocks
    scale2 = math.log2(math.e) / math.sqrt(width)
    count = list_ref[4, 0]
    groups = (count + GROUP - 1) // GROUP

    def copies(g, i):
        at = g * GROUP + i
        page = list_ref[2, at]
        slot = lax.rem(g, RING)
        return (
            pltpu.make_async_copy(keys.at[page], key_buf.at[slot, i], key_sem.at[slot, i]),
            pltpu.make_async_copy(values.at[page], value_buf.at[slot, i], value_sem.at[slot, i]),
        )

    def start(g):
        for i in range(GROUP):
            for copy in copies(g, i):
                copy.start()

    for g in range(RING - 1):
        pl.when(g < groups)(functools.partial(start, g))

    best[...] = jnp.full(best.shape, LOWEST_SCORE, jnp.float32)
    weight[...] = jnp.zeros(weight.shape, jnp.float32)
    total[...] = jnp.zeros(total.shape, jnp.float32)
    if q_ref.ndim == 4 and q_ref.shape[2] % group_rows == 0:
        each = q_ref.shape[2] // group_rows
        for d in range(q_ref.shape[0]):
            for h in range(heads):
                block = q_ref[d, h].astype(jnp.float32)
                for j in range(each):
                    q_wide[d * each + j, h] = block[j * group_rows : (j + 1) * group_rows]
    else:
        for d in range(q_ref.shape[0]):
            for h in range(heads):
                rows = q_ref.shape[2]
                parts = group_rows // rows
                q_wide[d // parts, h, (d % parts) * rows : (d % parts + 1) * rows] = q_ref[
                    d, h
                ].astype(jnp.float32)

    lane = lax.broadcasted_iota(jnp.int32, (group_rows, page_len), 1)

    def step(g, carry):
        pl.when(g + RING - 1 < groups)(lambda: start(g + RING - 1))
        slot = lax.rem(g, RING)
        for i in range(GROUP):
            for copy in copies(g, i):
                copy.wait()
        seq = [list_ref[0, g * GROUP + i] for i in range(GROUP)]
        inside = [lane < list_ref[3, g * GROUP + i] for i in range(GROUP)]
        both = [(i, pair) for i in range(GROUP) for pair in range(0, heads, 2)]
        each = [(i, h) for i in range(GROUP) for h in range(heads)]
        scores = {}
        for i, pair in both:
            q2 = q_wide[seq[i], pair : pair + 2].reshape(2 * group_rows, width)
            k2 = key_buf[slot, i, pair : pair + 2].reshape(2 * page_len, width)
            found = _dot(q2.astype(jnp.bfloat16), k2, NT)
            for e in range(2):
                scores[i, pair + e] = found[
                    e * group_rows : (e + 1) * group_rows, e * page_len : (e + 1) * page_len
                ]
        tops, lines = {}, {}
        for i, h in each:
            sc = jnp.where(inside[i], scores[i, h], LOWEST_SCORE)
            scores[i, h] = sc
            tops[i, h] = jnp.broadcast_to(jnp.max(sc, axis=1, keepdims=True), sc.shape)
        for i, h in each:
            lines[i, h] = jnp.where(
                inside[i], jnp.exp2((scores[i, h] - tops[i, h]) * scale2), 0.0
            )
        outs = {}
        for i, pair in both:
            w2 = jnp.concatenate([lines[i, pair], lines[i, pair + 1]], axis=0)
            v2 = jnp.concatenate(
                [value_buf[slot, i, pair], value_buf[slot, i, pair + 1]], axis=1
            )
            found = _dot(w2.astype(jnp.bfloat16), v2, NN)
            for e in range(2):
                outs[i, pair + e] = found[
                    e * group_rows : (e + 1) * group_rows, e * width : (e + 1) * width
                ]
        for i, h in each:
            s = seq[i]
            old = best[s, h]
            new = jnp.maximum(old, tops[i, h])
            keep = jnp.exp2((old - new) * scale2)
            add = jnp.exp2((tops[i, h] - new) * scale2)
            best[s, h] = new
            weight[s, h] = weight[s, h] * keep + lines[i, h] * add
            total[s, h] = total[s, h] * keep + outs[i, h] * add
        return carry

    lax.fori_loop(0, groups, step, 0)

    stat_lane = lax.broadcasted_iota(jnp.int32, (group_rows, width), 1)
    columns = heads * per_block
    for b in range(blocks):
        stats = jnp.zeros((group_rows, width), jnp.float32)
        for j in range(per_block):
            s = b * per_block + j
            for h in range(heads):
                at = h * per_block + j
                out_ref[b, at] = total[s, h]
                mass = jnp.sum(weight[s, h], axis=1, keepdims=True)
                stats = jnp.where(stat_lane == at, best[s, h], stats)
                stats = jnp.where(
                    stat_lane == columns + at, jnp.broadcast_to(mass, stats.shape), stats
                )
        out_ref[b, columns] = stats


def fold(pieces, columns, scale2):
    stats = [piece[columns] for piece in pieces]
    top = functools.reduce(jnp.maximum, stats)
    mass = jnp.zeros_like(top)
    sums = [jnp.zeros_like(top) for _ in range(columns)]
    for piece, own in zip(pieces, stats):
        factor = jnp.exp2((own - top) * scale2)
        mass = mass + own * pltpu.roll(factor, columns, 1)
        for c in range(columns):
            sums[c] = sums[c] + piece[c] * jnp.broadcast_to(factor[:, c : c + 1], top.shape)
    return top, mass, sums


def exchange_kernel(
    n,
    plane,
    parts,
    part_ref,
    q_ref,
    key_ref,
    value_ref,
    out_ref,
    near,
    folded,
    far,
    near_send,
    near_recv,
    far_send,
    far_recv,
    own_sem,
):
    me = lax.axis_index("kv")
    lines = n // plane
    spot, line = lax.rem(me, plane), me // plane
    tiles, group_rows, width = folded.shape[1:]
    columns = tiles - 1
    heads = q_ref.shape[0]
    per_block = columns // heads
    scale2 = math.log2(math.e) / math.sqrt(width)
    spots = [lax.rem(spot + k, plane) for k in range(1, plane)]
    turns = list(range(lines // 2, lines)) + list(range(lines // 2 - 1, 0, -1)) + [0]
    floors = [lax.rem(line + k, lines) for k in turns]
    own = []
    for k, floor in enumerate(floors):
        copy = pltpu.make_async_copy(
            part_ref.at[(floor * plane + spot) // parts], near.at[floor, spot], own_sem.at[k]
        )
        copy.start()
        own.append(copy)
    greet([line * plane + p for p in spots] + [f * plane + spot for f in floors[:-1]])
    copies = []
    for k, floor in enumerate(floors):
        for p, other in enumerate(spots):
            copy = pltpu.make_async_remote_copy(
                src_ref=part_ref.at[(floor * plane + other) // parts],
                dst_ref=near.at[floor, spot],
                send_sem=near_send.at[k, p],
                recv_sem=near_recv.at[floor, spot],
                device_id={"kv": line * plane + other},
                device_id_type=MESH,
            )
            copy.start()
            copies.append(copy)
    for k, floor in enumerate(floors):
        own[k].wait()
        for p, other in enumerate(spots):
            pltpu.make_async_remote_copy(
                src_ref=part_ref.at[(floor * plane + other) // parts],
                dst_ref=near.at[floor, other],
                send_sem=near_send.at[k, p],
                recv_sem=near_recv.at[floor, other],
                device_id={"kv": line * plane + other},
                device_id_type=MESH,
            ).wait_recv()
        top, mass, sums = fold([near.at[floor, p] for p in range(plane)], columns, scale2)
        stat_lane = lax.broadcasted_iota(jnp.int32, top.shape, 1)
        stats = jnp.where(stat_lane < columns, top, mass)
        for c in range(columns):
            folded[k, c] = sums[c]
        folded[k, columns] = stats
        if k < lines - 1:
            copy = pltpu.make_async_remote_copy(
                src_ref=folded.at[k],
                dst_ref=far.at[line],
                send_sem=far_send.at[k],
                recv_sem=far_recv.at[line],
                device_id={"kv": floor * plane + spot},
                device_id_type=MESH,
            )
            copy.start()
            copies.append(copy)
    for k, floor in enumerate(floors[:-1]):
        pltpu.make_async_remote_copy(
            src_ref=folded.at[k],
            dst_ref=far.at[floor],
            send_sem=far_send.at[k],
            recv_sem=far_recv.at[floor],
            device_id={"kv": floor * plane + spot},
            device_id_type=MESH,
        ).wait_recv()
    top, mass, sums = fold(
        [folded.at[lines - 1]] + [far.at[floor] for floor in floors[:-1]], columns, scale2
    )
    for h in range(heads):
        wide = q_ref[h].astype(jnp.float32)
        results = []
        for j in range(per_block):
            c = h * per_block + j
            s = (me // parts) * per_block + j
            rows = slice(j * group_rows, (j + 1) * group_rows) if parts == 1 else slice(None)
            query = wide[rows]
            shape = query.shape
            fresh_key = jnp.broadcast_to(key_ref[s][h : h + 1].astype(jnp.float32), shape)
            fresh_value = jnp.broadcast_to(value_ref[s][h : h + 1].astype(jnp.float32), shape)
            new = jnp.broadcast_to(jnp.sum(query * fresh_key, axis=1, keepdims=True), shape)

            def mine(x):
                if parts == 1:
                    return x
                size = group_rows // parts
                picked = x[:size]
                for p in range(1, parts):
                    picked = jnp.where(
                        lax.rem(me, parts) == p, x[p * size : (p + 1) * size], picked
                    )
                return picked

            old = mine(jnp.broadcast_to(top[:, c : c + 1], top.shape))
            old_mass = mine(jnp.broadcast_to(mass[:, columns + c : columns + c + 1], top.shape))
            old_sum = mine(sums[c])
            highest = jnp.maximum(old, new)
            old_part = jnp.exp2((old - highest) * scale2)
            new_part = jnp.exp2((new - highest) * scale2)
            results.append(
                (old_sum * old_part + new_part * fresh_value) / (old_mass * old_part + new_part)
            )
        out_ref[h] = jnp.concatenate(results, axis=0).astype(out_ref.dtype)
    for copy in copies:
        copy.wait_send()


def on_device(n, queries, key_cache, value_cache, key_new, value_new, lengths, page_table):
    heads, local_rows, width = queries.shape
    seqs = lengths.shape[0]
    slots = page_table.shape[0] // seqs
    pages_here, _, page_len, _ = key_cache.shape
    group_rows = local_rows * n // seqs
    parts = max(1, group_rows // local_rows)
    blocks = n // parts
    tiles = heads * (seqs // blocks) + 1
    listed = -(-pages_here // 128) * 128 + 128
    vmem = pl.BlockSpec(memory_space=VMEM)
    smem = pl.BlockSpec(memory_space=pltpu.SMEM)
    hbm = pl.BlockSpec(memory_space=pl.ANY)

    every_query, pages = pl.pallas_call(
        functools.partial(gather_kernel, n, pages_here, page_len),
        out_shape=(
            jax.ShapeDtypeStruct((n,) + queries.shape, queries.dtype),
            jax.ShapeDtypeStruct((8, listed), jnp.int32),
        ),
        in_specs=[vmem, vmem, smem],
        out_specs=(vmem, vmem),
        scratch_shapes=[
            pltpu.SemaphoreType.DMA((n,)),
            pltpu.SemaphoreType.DMA((n,)),
            pltpu.SemaphoreType.DMA,
        ],
        compiler_params=pltpu.CompilerParams(
            collective_id=0, has_side_effects=True, vmem_limit_bytes=16 * 1024 * 1024
        ),
        name="gather_queries",
    )(queries, page_table.reshape(seqs, slots), lengths)

    part = pl.pallas_call(
        functools.partial(attend_kernel, group_rows, blocks),
        out_shape=jax.ShapeDtypeStruct((blocks, tiles, group_rows, width), jnp.float32),
        in_specs=[smem, vmem, hbm, hbm],
        out_specs=vmem,
        scratch_shapes=[
            VMEM((seqs, heads, group_rows, width), jnp.float32),
            VMEM((RING, GROUP, heads, page_len, width), key_cache.dtype),
            VMEM((RING, GROUP, heads, page_len, width), value_cache.dtype),
            VMEM((seqs, heads, group_rows, page_len), jnp.float32),
            VMEM((seqs, heads, group_rows, page_len), jnp.float32),
            VMEM((seqs, heads, group_rows, width), jnp.float32),
            pltpu.SemaphoreType.DMA((RING, GROUP)),
            pltpu.SemaphoreType.DMA((RING, GROUP)),
        ],
        compiler_params=pltpu.CompilerParams(vmem_limit_bytes=48 * 1024 * 1024),
        name="attend_pages",
    )(pages, every_query, key_cache, value_cache)

    plane = min(p for p in range(1, n + 1) if n % p == 0 and p * p >= n)
    lines = n // plane
    tile = (tiles, group_rows, width)
    return pl.pallas_call(
        functools.partial(exchange_kernel, n, plane, parts),
        out_shape=jax.ShapeDtypeStruct(queries.shape, jnp.bfloat16),
        in_specs=[vmem] + [vmem] * 3,
        out_specs=vmem,
        scratch_shapes=[
            VMEM((lines, plane) + tile, jnp.float32),
            VMEM((lines,) + tile, jnp.float32),
            VMEM((lines,) + tile, jnp.float32),
            pltpu.SemaphoreType.DMA((lines, plane)),
            pltpu.SemaphoreType.DMA((lines, plane)),
            pltpu.SemaphoreType.DMA((lines,)),
            pltpu.SemaphoreType.DMA((lines,)),
            pltpu.SemaphoreType.DMA((lines,)),
        ],
        compiler_params=pltpu.CompilerParams(
            collective_id=1, has_side_effects=True, vmem_limit_bytes=16 * 1024 * 1024
        ),
        name="exchange_and_finish",
    )(part, queries, key_new, value_new)


def solution(mesh):
    placed = (
        P("head", "kv", None),
        P("kv", "head", None, None),
        P("kv", "head", None, None),
        P(None, "head", None),
        P(None, "head", None),
        P(),
        P(),
    )
    return jax.shard_map(
        functools.partial(on_device, mesh.shape["kv"]),
        mesh=mesh,
        in_specs=placed,
        out_specs=P("head", "kv", None),
        check_vma=False,
    )
```
